16 devices in a mesh: rep: 1, dp: 16 (over x, y, z, core).
Axes of the slice: x: 2, y: 2, z: 2, core: 2. Of those that a mesh axis runs over, the one named last changes fastest.
Arguments:
- x: bfloat16 [16, 2048, 1024], P(('rep', 'dp'))
- dy: bfloat16 [16, 2048, 1024], P(('rep', 'dp'))
- w_gate: bfloat16 [2, 1024, 2560], replicated
- w_up: bfloat16 [2, 1024, 2560], replicated
- w_down: bfloat16 [2, 2560, 1024], replicated
- m_w_gate: float32 [2, 1024, 2560], replicated
- m_w_up: float32 [2, 1024, 2560], replicated
- m_w_down: float32 [2, 2560, 1024], replicated
- v_w_gate: float32 [2, 1024, 2560], replicated
- v_w_up: float32 [2, 1024, 2560], replicated
- v_w_down: float32 [2, 2560, 1024], replicated
Outputs:
- output 1: bfloat16 [2, 1024, 2560], P('rep')
- output 2: bfloat16 [2, 1024, 2560], P('rep')
- output 3: bfloat16 [2, 2560, 1024], P('rep')
- output 4: float32 [2, 1024, 2560], P('rep')
- output 5: float32 [2, 1024, 2560], P('rep')
- output 6: float32 [2, 2560, 1024], P('rep')
- output 7: float32 [2, 1024, 2560], P('rep')
- output 8: float32 [2, 1024, 2560], P('rep')
- output 9: float32 [2, 2560, 1024], P('rep')
All inputs are finite; a program needn't handle non-finite values.
Results may differ from the reference program's by a relative error of at most 0.022.
Values are sent between devices in bfloat16 or wider.
A program may use at most 2.5 GiB of HBM per device.

```python
import jax
import jax.numpy as jnp
from jax import lax

SEQUENCES = 16
TOKENS = 2048
D = 1024
FF = 2560
LAYERS = 2
NAMES = ("w_gate", "w_up", "w_down")
SHAPES = {"w_gate": (LAYERS, D, FF), "w_up": (LAYERS, D, FF), "w_down": (LAYERS, FF, D)}


def bump(key, n, height):
    away = (jnp.arange(n, dtype=jnp.int32) - jax.random.randint(key, (), 0, n, jnp.int32)) % n
    return jnp.where(away < n // 8, height, 1.0)


def together(key, own, strength):
    shared = jax.random.normal(key, own.shape[1:], jnp.float32)
    return (own + strength * shared) * lax.rsqrt(1 + strength * strength)


def setup_inputs(seed: int = 0, part: int = 0) -> dict:
    kx, kdy, ka, kb, kz, kf, kh, kl, *keys = jax.random.split(jax.random.key(seed), 8 + 3 * len(NAMES))
    kx, kdy, ka, kb = (jax.random.fold_in(k, part) for k in (kx, kdy, ka, kb))
    kw, km, kv = (keys[i::3] for i in range(3))
    shape = (SEQUENCES, TOKENS, D)
    much_x, much_dy = jax.random.uniform(kz, (2,), jnp.float32, 0.0, 1.0)
    loud = 2.0 ** jax.random.uniform(jax.random.fold_in(kz, 1), (), jnp.float32, -1.0, 2.0)
    layers = 2.0 ** jax.random.uniform(kl, (LAYERS, 1, 1), jnp.float32, -1.0, 1.0)
    x = together(ka, jax.random.normal(kx, shape, jnp.float32), much_x) * bump(kf, D, 4.0)
    dy = together(kb, jax.random.normal(kdy, shape, jnp.float32), much_dy)
    drawn = {"x": x.astype(jnp.bfloat16), "dy": (loud * dy * (SEQUENCES * TOKENS) ** -0.5).astype(jnp.bfloat16)}
    for key, name in zip(kw, NAMES, strict=True):
        w = jax.random.normal(key, SHAPES[name], jnp.float32) * SHAPES[name][1] ** -0.5
        drawn[name] = (w * {"w_gate": 1.0, "w_up": bump(kh, FF, 4.0), "w_down": layers}[name]).astype(jnp.bfloat16)
    for key, name in zip(km, NAMES, strict=True):
        drawn[f"m_{name}"] = 0.1 * jax.random.normal(key, SHAPES[name], jnp.float32)
    for key, name in zip(kv, NAMES, strict=True):
        drawn[f"v_{name}"] = jax.random.uniform(key, SHAPES[name], jnp.float32, 0.005, 0.015)
    return drawn


def matmul(a, w):
    return jnp.dot(a, w, preferred_element_type=jnp.float32).astype(jnp.bfloat16)


def normed(h):
    wide = h.astype(jnp.float32)
    scale = lax.rsqrt(jnp.mean(wide**2, -1, keepdims=True) + 1e-6)
    return (wide * scale).astype(jnp.bfloat16)


def layer(h, w):
    a = normed(h)
    gate = jnp.dot(a, w["w_gate"], preferred_element_type=jnp.float32)
    up = jnp.dot(a, w["w_up"], preferred_element_type=jnp.float32)
    return h + matmul((jax.nn.silu(gate) * up).astype(jnp.bfloat16), w["w_down"])


def adamw(w, m, v, g):
    m = 0.9 * m + 0.1 * g
    v = 0.95 * v + 0.05 * g * g
    step = m * lax.rsqrt(v + 1e-8) + 0.1 * w
    return (w - 0.02 * step).astype(jnp.bfloat16), m, v


def clipped(gradients, sum_of_squares, count):
    factor = jnp.minimum(1.0, 0.5 * lax.rsqrt(sum_of_squares / count + 1e-30))
    return [g * factor for g in gradients]


def stack(weights, h):
    return lax.scan(lambda h, w: (layer(h, w), None), h, weights)[0]


def reference(x, dy, w_gate, w_up, w_down, m_w_gate, m_w_up, m_w_down, v_w_gate, v_w_up, v_w_down):
    weights = dict(zip(NAMES, (w_gate, w_up, w_down), strict=True))

    def take(so_far, sequence):
        h, by_y = sequence
        _, back = jax.vjp(lambda w: stack(w, h), weights)
        return jax.tree.map(lambda total, term: total + term.astype(jnp.float32), so_far, back(by_y)[0]), None

    none_yet = {name: jnp.zeros(w.shape, jnp.float32) for name, w in weights.items()}
    by_weights, _ = lax.scan(take, none_yet, (x, dy))
    gradients = [by_weights[name].astype(jnp.bfloat16).astype(jnp.float32) for name in NAMES]
    gradients = clipped(gradients, sum(jnp.sum(g * g) for g in gradients), sum(g.size for g in gradients))
    new = [
        adamw(w.astype(jnp.float32), m, v, g)
        for w, m, v, g in zip((w_gate, w_up, w_down), (m_w_gate, m_w_up, m_w_down), (v_w_gate, v_w_up, v_w_down), gradients, strict=True)
    ]
    return tuple(one[which] for which in range(3) for one in new)
```

```python
import functools
import jax
import jax.numpy as jnp
from jax import lax
from jax.experimental import pallas as pl
from jax.experimental.pallas import tpu as pltpu
from jax.sharding import PartitionSpec as P

T, D, F = 2048, 1024, 2560
FT = 512
NT = F // FT
MB = 512
BF, F32 = jnp.bfloat16, jnp.float32
VL = 64 * 1024 * 1024 - 128 * 1024
NN = (((1,), (0,)), ((), ()))
NTR = (((1,), (1,)), ((), ()))


def dot(a, b, dims=NN):
    return lax.dot_general(a, b, dims, preferred_element_type=F32)


def params():
    return pltpu.CompilerParams(vmem_limit_bytes=VL, dimension_semantics=("arbitrary",))


def norm_block(h):
    wide = h.astype(F32)
    scale = lax.rsqrt(jnp.mean(wide * wide, -1, keepdims=True) + 1e-6)
    return (wide * scale).astype(BF)


def rows(i, n):
    return pl.ds(pl.multiple_of(i * n, n), n)


def norm_into(h_ref, a_ref, at_ref, n=256):
    def body(i, _):
        a = norm_block(h_ref[rows(i, n), :])
        if a_ref is not None:
            a_ref[rows(i, n), :] = a
        if at_ref is not None:
            at_ref[:, rows(i, n)] = a.T
        return 0
    lax.fori_loop(0, T // n, body, 0)


def transpose_into(h_ref, at_ref, n=256):
    def body(i, _):
        at_ref[:, rows(i, n)] = h_ref[rows(i, n), :].T
        return 0
    lax.fori_loop(0, T // n, body, 0)


def kernel_a(x_ref, wg_ref, wu_ref, wd_ref, gate_ref, up_ref, h1_ref, a_ref, acc_ref):
    t = pl.program_id(0)

    @pl.when(t == 0)
    def _():
        norm_into(x_ref, a_ref, None)

    def body(first, i, _):
        r = rows(i, MB)
        a = a_ref[r, :]
        gate = dot(a, wg_ref[0])
        up = dot(a, wu_ref[0])
        gate_ref[r, :] = gate
        up_ref[r, :] = up
        hid = (gate * jax.nn.sigmoid(gate) * up).astype(BF)
        y = dot(hid, wd_ref[0])
        if first:
            acc_ref[r, :] = y
        else:
            acc_ref[r, :] += y
        return 0

    @pl.when(t == 0)
    def _():
        lax.fori_loop(0, T // MB, functools.partial(body, True), 0)

    @pl.when(t > 0)
    def _():
        lax.fori_loop(0, T // MB, functools.partial(body, False), 0)

    @pl.when(t == NT - 1)
    def _():
        def fin(i, _):
            r = rows(i, MB)
            h1_ref[r, :] = (x_ref[r, :].astype(F32) + acc_ref[r, :].astype(BF).astype(F32)).astype(BF)
            return 0
        lax.fori_loop(0, T // MB, fin, 0)


def forward0(x, wg, wu, wd):
    whole = pl.BlockSpec((T, D), lambda t: (0, 0), pipeline_mode=pl.Buffered(1))
    return pl.pallas_call(
        kernel_a,
        grid=(NT,),
        in_specs=[whole,
                  pl.BlockSpec((1, D, FT), lambda t: (0, 0, t)),
                  pl.BlockSpec((1, D, FT), lambda t: (0, 0, t)),
                  pl.BlockSpec((1, FT, D), lambda t: (0, t, 0))],
        out_specs=[pl.BlockSpec((T, FT), lambda t: (0, t)), pl.BlockSpec((T, FT), lambda t: (0, t)), pl.BlockSpec((T, D), lambda t: (0, 0))],
        out_shape=[jax.ShapeDtypeStruct((T, F), F32), jax.ShapeDtypeStruct((T, F), F32), jax.ShapeDtypeStruct((T, D), BF)],
        scratch_shapes=[pltpu.VMEM((T, D), BF), pltpu.VMEM((T, D), F32)],
        compiler_params=params(),
        cost_estimate=pl.CostEstimate(flops=6 * T * D * F, bytes_accessed=8 * T * F + 6 * D * F, transcendentals=0),
        name="fwd0",
    )(x, wg, wu, wd)


def back_elementwise(gate, up, dhid):
    s = jax.nn.sigmoid(gate)
    silu = gate * s
    dh = dhid.astype(BF).astype(F32)
    hid = (silu * up).astype(BF)
    du = (dh * silu).astype(BF)
    dg = (dh * up * (s + silu * (1.0 - s))).astype(BF)
    return hid, dg, du


def weight_grads(at_ref, dt_ref, hid_ref, dg_ref, du_ref, g_ref):
    def body(n, _):
        r = rows(n, 256)
        at = at_ref[r, :]
        g_ref[0, r, :] = dot(at, dg_ref[...]).astype(BF)
        g_ref[1, r, :] = dot(at, du_ref[...]).astype(BF)
        g_ref[2, r, :] = dot(dt_ref[r, :], hid_ref[...]).astype(BF)
        return 0
    lax.fori_loop(0, D // 256, body, 0)


def kernel_b(h_ref, dy_ref, wg_ref, wu_ref, wd_ref, g_ref, dh_ref, a_ref, at_ref, dt_ref, accg_ref, accu_ref, hid_ref, dg_ref, du_ref):
    t = pl.program_id(0)

    @pl.when(t == 0)
    def _():
        norm_into(h_ref, a_ref, at_ref)
        transpose_into(dy_ref, dt_ref)

    def body(first, i, _):
        r = rows(i, MB)
        a = a_ref[r, :]
        gate = dot(a, wg_ref[0])
        up = dot(a, wu_ref[0])
        dhid = dot(dy_ref[r, :], wd_ref[0], NTR)
        hid, dg, du = back_elementwise(gate, up, dhid)
        hid_ref[r, :] = hid
        dg_ref[r, :] = dg
        du_ref[r, :] = du
        yg = dot(dg, wg_ref[0], NTR)
        yu = dot(du, wu_ref[0], NTR)
        if first:
            accg_ref[r, :] = yg
            accu_ref[r, :] = yu
        else:
            accg_ref[r, :] += yg
            accu_ref[r, :] += yu
        return 0

    @pl.when(t == 0)
    def _():
        lax.fori_loop(0, T // MB, functools.partial(body, True), 0)

    @pl.when(t > 0)
    def _():
        lax.fori_loop(0, T // MB, functools.partial(body, False), 0)

    weight_grads(at_ref, dt_ref, hid_ref, dg_ref, du_ref, g_ref)

    @pl.when(t == NT - 1)
    def _():
        def fin(i, _):
            r = rows(i, 256)
            wide = h_ref[r, :].astype(F32)
            scale = lax.rsqrt(jnp.mean(wide * wide, -1, keepdims=True) + 1e-6)
            da = (accg_ref[r, :].astype(BF).astype(F32) + accu_ref[r, :].astype(BF).astype(F32)).astype(BF).astype(F32)
            inner = jnp.mean(da * wide, -1, keepdims=True)
            dn = (da * scale - wide * (scale * scale * scale * inner)).astype(BF).astype(F32)
            dh_ref[r, :] = (dy_ref[r, :].astype(F32) + dn).astype(BF)
            return 0
        lax.fori_loop(0, T // 256, fin, 0)


def layer1(h1, dy, wg, wu, wd):
    whole = pl.BlockSpec((T, D), lambda t: (0, 0), pipeline_mode=pl.Buffered(1))
    return pl.pallas_call(
        kernel_b,
        grid=(NT,),
        in_specs=[whole, whole,
                  pl.BlockSpec((1, D, FT), lambda t: (1, 0, t)),
                  pl.BlockSpec((1, D, FT), lambda t: (1, 0, t)),
                  pl.BlockSpec((1, FT, D), lambda t: (1, t, 0))],
        out_specs=[pl.BlockSpec((3, D, FT), lambda t: (0, 0, t)), pl.BlockSpec((T, D), lambda t: (0, 0), pipeline_mode=pl.Buffered(1))],
        out_shape=[jax.ShapeDtypeStruct((3, D, F), BF), jax.ShapeDtypeStruct((T, D), BF)],
        scratch_shapes=[pltpu.VMEM((T, D), BF), pltpu.VMEM((D, T), BF), pltpu.VMEM((D, T), BF), pltpu.VMEM((T, D), F32), pltpu.VMEM((T, D), F32),
                        pltpu.VMEM((T, FT), BF), pltpu.VMEM((T, FT), BF), pltpu.VMEM((T, FT), BF)],
        compiler_params=params(),
        cost_estimate=pl.CostEstimate(flops=16 * T * D * F, bytes_accessed=12 * D * F + 6 * T * D, transcendentals=0),
        name="layer1",
    )(h1, dy, wg, wu, wd)


def kernel_c(x_ref, dh_ref, gate_ref, up_ref, wd_ref, g_ref, at_ref, dt_ref, hid_ref, dg_ref, du_ref):
    t = pl.program_id(0)

    @pl.when(t == 0)
    def _():
        norm_into(x_ref, None, at_ref)
        transpose_into(dh_ref, dt_ref)

    def body(i, _):
        r = rows(i, MB)
        dhid = dot(dh_ref[r, :], wd_ref[0], NTR)
        hid, dg, du = back_elementwise(gate_ref[r, :], up_ref[r, :], dhid)
        hid_ref[r, :] = hid
        dg_ref[r, :] = dg
        du_ref[r, :] = du
        return 0
    lax.fori_loop(0, T // MB, body, 0)
    weight_grads(at_ref, dt_ref, hid_ref, dg_ref, du_ref, g_ref)


def back0(x, dh1, gate, up, wd):
    whole = pl.BlockSpec((T, D), lambda t: (0, 0), pipeline_mode=pl.Buffered(1))
    return pl.pallas_call(
        kernel_c,
        grid=(NT,),
        in_specs=[whole, whole, pl.BlockSpec((T, FT), lambda t: (0, t)), pl.BlockSpec((T, FT), lambda t: (0, t)),
                  pl.BlockSpec((1, FT, D), lambda t: (0, t, 0))],
        out_specs=pl.BlockSpec((3, D, FT), lambda t: (0, 0, t)),
        out_shape=jax.ShapeDtypeStruct((3, D, F), BF),
        scratch_shapes=[pltpu.VMEM((D, T), BF), pltpu.VMEM((D, T), BF),
                        pltpu.VMEM((T, FT), BF), pltpu.VMEM((T, FT), BF), pltpu.VMEM((T, FT), BF)],
        compiler_params=params(),
        cost_estimate=pl.CostEstimate(flops=8 * T * D * F, bytes_accessed=8 * T * F + 8 * D * F, transcendentals=0),
        name="back0",
    )(x, dh1, gate, up, wd)


def adamw_into(w_ref, m_ref, v_ref, g, wo_ref, mo_ref, vo_ref):
    m = 0.9 * m_ref[0] + 0.1 * g
    v = 0.95 * v_ref[0] + 0.05 * g * g
    w = w_ref[0].astype(F32)
    wo_ref[0] = (w - 0.02 * (m * lax.rsqrt(v + 1e-8) + 0.1 * w)).astype(BF)
    mo_ref[0] = m
    vo_ref[0] = v


def kernel_o(f_ref, g_ref, *refs):
    ins, outs = refs[:9], refs[-9:]
    factor = f_ref[0, 0]
    for i in range(3):
        g = g_ref[i].astype(F32)
        if i == 2:
            g = g.T
        adamw_into(ins[i], ins[3 + i], ins[6 + i], g * factor, outs[i], outs[3 + i], outs[6 + i])


def optimizer(layer, factor, g, arrays, before):
    fb = 256
    wide = pl.BlockSpec((1, D, fb), lambda t: (layer, 0, t))
    tall = pl.BlockSpec((1, fb, D), lambda t: (layer, t, 0))
    three = [wide, wide, tall]
    alias = {} if before is None else {11 + i: i for i in range(9)}
    return pl.pallas_call(
        kernel_o,
        grid=(F // fb,),
        in_specs=[pl.BlockSpec(memory_space=pltpu.SMEM), pl.BlockSpec((3, D, fb), lambda t: (0, 0, t))] + three * 3
        + ([] if before is None else [pl.BlockSpec(memory_space=pl.ANY)] * 9),
        out_specs=three * 3,
        out_shape=[jax.ShapeDtypeStruct(a.shape, a.dtype) for a in arrays],
        input_output_aliases=alias,
        compiler_params=params(),
        cost_estimate=pl.CostEstimate(flops=30 * D * F, bytes_accessed=66 * D * F, transcendentals=3 * D * F),
        name=f"adamw{layer}",
    )(factor, g, *arrays, *(before or ()))


def solution(mesh):
    def step(x, dy, *arrays):
        wg, wu, wd = arrays[:3]
        gate, up, h1 = forward0(x[0], wg, wu, wd)
        g1, dh1 = layer1(h1, dy[0], wg, wu, wd)
        s1 = lax.psum_scatter(g1.reshape(3 * D, F), "dp", scatter_dimension=0, tiled=True)
        g0 = back0(x[0], dh1, gate, up, wd)
        g0, s1 = lax.optimization_barrier((g0, s1))
        s0 = lax.psum_scatter(g0.reshape(3 * D, F), "dp", scatter_dimension=0, tiled=True)
        squares = lax.psum(sum(jnp.sum(s.astype(F32) ** 2) for s in (s0, s1)), "dp")
        factor = jnp.minimum(1.0, 0.5 * lax.rsqrt(squares / (6 * D * F) + 1e-30)).reshape(1, 1)
        a1 = lax.all_gather(s1, "dp", axis=0, tiled=True)
        a0 = lax.all_gather(s0, "dp", axis=0, tiled=True)
        out = optimizer(1, factor, a1.reshape(3, D, F), arrays, None)
        return tuple(optimizer(0, factor, a0.reshape(3, D, F), arrays, out))

    return jax.shard_map(
        step,
        mesh=mesh,
        in_specs=(P(("rep", "dp"), None, None),) * 2 + (P(None, None, None),) * 9,
        out_specs=(P("rep", None, None),) * 9,
        check_vma=False,
    )
```

```python
import functools
import jax
import jax.numpy as jnp
from jax import lax
from jax.experimental import pallas as pl
from jax.experimental.pallas import tpu as pltpu
from jax.sharding import PartitionSpec as P

T, D, F = 2048, 1024, 2560
FT = 512
NT = F // FT
MB = 512
BF, F32 = jnp.bfloat16, jnp.float32
VL = 64 * 1024 * 1024 - 128 * 1024
NN = (((1,), (0,)), ((), ()))
NTR = (((1,), (1,)), ((), ()))


def dot(a, b, dims=NN):
    return lax.dot_general(a, b, dims, preferred_element_type=F32)


def params(**more):
    return pltpu.CompilerParams(vmem_limit_bytes=VL, dimension_semantics=("arbitrary",), **more)


def norm_block(h):
    wide = h.astype(F32)
    scale = lax.rsqrt(jnp.mean(wide * wide, -1, keepdims=True) + 1e-6)
    return (wide * scale).astype(BF)


def rows(i, n):
    return pl.ds(pl.multiple_of(i * n, n), n)


def norm_into(h_ref, a_ref, at_ref, n=256):
    def body(i, _):
        a = norm_block(h_ref[rows(i, n), :])
        if a_ref is not None:
            a_ref[rows(i, n), :] = a
        if at_ref is not None:
            at_ref[:, rows(i, n)] = a.T
        return 0
    lax.fori_loop(0, T // n, body, 0)


def transpose_into(h_ref, at_ref, n=256):
    def body(i, _):
        at_ref[:, rows(i, n)] = h_ref[rows(i, n), :].T
        return 0
    lax.fori_loop(0, T // n, body, 0)


def kernel_a(x_ref, wg_ref, wu_ref, wd_ref, gate_ref, up_ref, h1_ref, at_ref, a_ref, acc_ref):
    t = pl.program_id(0)

    @pl.when(t == 0)
    def _():
        norm_into(x_ref, a_ref, at_ref)

    def body(first, i, _):
        r = rows(i, MB)
        a = a_ref[r, :]
        gate = dot(a, wg_ref[0])
        up = dot(a, wu_ref[0])
        gate_ref[r, :] = gate
        up_ref[r, :] = up
        hid = (gate * jax.nn.sigmoid(gate) * up).astype(BF)
        y = dot(hid, wd_ref[0])
        if first:
            acc_ref[r, :] = y
        else:
            acc_ref[r, :] += y
        return 0

    @pl.when(t == 0)
    def _():
        lax.fori_loop(0, T // MB, functools.partial(body, True), 0)

    @pl.when(t > 0)
    def _():
        lax.fori_loop(0, T // MB, functools.partial(body, False), 0)

    @pl.when(t == NT - 1)
    def _():
        def fin(i, _):
            r = rows(i, MB)
            h1_ref[r, :] = (x_ref[r, :].astype(F32) + acc_ref[r, :].astype(BF).astype(F32)).astype(BF)
            return 0
        lax.fori_loop(0, T // MB, fin, 0)


def forward0(x, wg, wu, wd):
    whole = pl.BlockSpec((T, D), lambda t: (0, 0), pipeline_mode=pl.Buffered(1))
    return pl.pallas_call(
        kernel_a,
        grid=(NT,),
        in_specs=[whole,
                  pl.BlockSpec((1, D, FT), lambda t: (0, 0, t)),
                  pl.BlockSpec((1, D, FT), lambda t: (0, 0, t)),
                  pl.BlockSpec((1, FT, D), lambda t: (0, t, 0))],
        out_specs=[pl.BlockSpec((T, FT), lambda t: (0, t)), pl.BlockSpec((T, FT), lambda t: (0, t)), whole,
                   pl.BlockSpec((D, T), lambda t: (0, 0), pipeline_mode=pl.Buffered(1))],
        out_shape=[jax.ShapeDtypeStruct((T, F), F32), jax.ShapeDtypeStruct((T, F), F32), jax.ShapeDtypeStruct((T, D), BF),
                   jax.ShapeDtypeStruct((D, T), BF)],
        scratch_shapes=[pltpu.VMEM((T, D), BF), pltpu.VMEM((T, D), F32)],
        compiler_params=params(),
        cost_estimate=pl.CostEstimate(flops=6 * T * D * F, bytes_accessed=8 * T * F + 6 * D * F, transcendentals=0),
        name="fwd0",
    )(x, wg, wu, wd)


def back_elementwise(gate, up, dhid):
    s = jax.nn.sigmoid(gate)
    silu = gate * s
    dh = dhid.astype(BF).astype(F32)
    hid = (silu * up).astype(BF)
    du = (dh * silu).astype(BF)
    dg = (dh * up * (s + silu * (1.0 - s))).astype(BF)
    return hid, dg, du


def weight_grads(at_ref, dt_ref, hid_ref, dg_ref, du_ref, g_ref, slot, lo, hi):
    def body(n, _):
        r = rows(n, 256)
        at = at_ref[r, :]
        g_ref[slot, 0, r, :] = dot(at, dg_ref[...]).astype(BF)
        g_ref[slot, 1, r, :] = dot(at, du_ref[...]).astype(BF)
        g_ref[slot, 2, r, :] = dot(dt_ref[r, :], hid_ref[...]).astype(BF)
        return 0
    lax.fori_loop(lo, hi, body, 0)


CORE = 1
ORDER = ((8, 4, 2), (4, 2, 8), (2, 8, 4))
PARTNERS = (1, 2, 4, 8)
HALVES = (512, 256, 128, 64)


def bit(stride):
    return (lax.axis_index("dp") // stride) % 2


def partner(stride):
    return {"dp": lax.axis_index("dp") + stride * (1 - 2 * bit(stride))}


def greet():
    barrier = pltpu.get_barrier_semaphore()
    for stride in PARTNERS:
        pl.semaphore_signal(barrier, inc=1, device_id=partner(stride), device_id_type=pl.DeviceIdType.MESH)
    pl.semaphore_wait(barrier, len(PARTNERS))


def some(start, n):
    return pl.ds(pl.multiple_of(start, 64), n)


def strides(c):
    return (CORE,) + ORDER[c]


class Scatter:
    def __init__(self, g, got, sent, send_sem, recv_sem):
        self.g, self.got, self.sent, self.send_sem, self.recv_sem = g, got, sent, send_sem, recv_sem

    def total(self, slot, c, stage, own):
        bits = [bit(s) for s in strides(c)]
        n = HALVES[stage] if stage < 4 else 64
        last = bits[stage] if own else 1 - bits[stage]
        keep = bits[:stage] + [last]
        start = sum(b * HALVES[i] for i, b in enumerate(keep))
        out = self.g[slot, c, some(start, n), :].astype(F32)
        for i in range(stage):
            start = sum(b * HALVES[j] for j, b in enumerate(keep) if j > i)
            out = out + self.got[i][slot, c, some(start, n), :].astype(F32)
        return out

    def copy(self, slot, c, stage):
        n = HALVES[stage]
        src = self.g.at[slot, c, some((1 - bit(CORE)) * 512, 512), :] if stage == 0 else self.sent[stage - 1].at[slot, c]
        return pltpu.make_async_remote_copy(
            src_ref=src, dst_ref=self.got[stage].at[slot, c], send_sem=self.send_sem.at[stage, c, slot], recv_sem=self.recv_sem.at[stage, c, slot],
            device_id=partner(strides(c)[stage]), device_id_type=pl.DeviceIdType.MESH)

    def begin(self, slot):
        for c in range(3):
            self.copy(slot, c, 0).start()

    def advance(self, slot, stage):
        for c in range(3):
            self.copy(slot, c, stage - 1).wait_recv()
            self.sent[stage - 1][slot, c] = self.total(slot, c, stage, False).astype(BF)
            self.copy(slot, c, stage).start()

    def finish(self, slot, shard, squares_ref):
        for c in range(3):
            self.copy(slot, c, 3).wait_recv()
            bits = [bit(s) for s in strides(c)]
            start = sum(b * HALVES[i] for i, b in enumerate(bits))
            out = self.g[slot, c, some(start, 64), :].astype(F32)
            for i in range(4):
                start = sum(b * HALVES[j] for j, b in enumerate(bits) if j > i)
                out = out + self.got[i][slot, c, some(start, 64), :].astype(F32)
            out = out.astype(BF)
            shard[c] = out
            squares = out.astype(F32) * out.astype(F32)
            squares_ref[...] += sum(squares[8 * i:8 * i + 8, 128 * j:128 * j + 128] for i in range(8) for j in range(FT // 128))
            for stage in range(4):
                self.copy(slot, c, stage).wait_send()


class Gather:
    def __init__(self, shards, full, own_sem, send_sem, recv_sem):
        self.shards, self.full, self.own_sem, self.send_sem, self.recv_sem = shards, full, own_sem, send_sem, recv_sem

    def place(self, tile, c, n):
        start = sum(bit(s) * HALVES[i] for i, s in enumerate(strides(c)) if HALVES[i] >= n)
        return self.full.at[c, some(start, n), pl.ds(pl.multiple_of(tile * FT, FT), FT)]

    def own(self, tile, c):
        return pltpu.make_async_copy(self.shards.at[tile, c], self.place(tile, c, 64), self.own_sem.at[tile, c])

    def copy(self, tile, c, stage):
        place = self.place(tile, c, 64 << stage)
        return pltpu.make_async_remote_copy(
            src_ref=self.shards.at[tile, c] if stage == 0 else place, dst_ref=place,
            send_sem=self.send_sem.at[tile, stage, c], recv_sem=self.recv_sem.at[tile, stage, c],
            device_id=partner(strides(c)[3 - stage]), device_id_type=pl.DeviceIdType.MESH)

    def begin(self, tile):
        for c in range(3):
            self.own(tile, c).start()
            self.copy(tile, c, 0).start()

    def advance(self, tile, stage):
        for c in range(3):
            if stage == 1:
                self.own(tile, c).wait()
            self.copy(tile, c, stage - 1).wait_recv()
            self.copy(tile, c, stage).start()

    def finish(self, tile):
        for c in range(3):
            self.copy(tile, c, 3).wait_recv()
            for stage in range(4):
                self.copy(tile, c, stage).wait_send()


def gather_scratch(tiles):
    return [pltpu.SemaphoreType.DMA((tiles, 3)), pltpu.SemaphoreType.DMA((tiles, 4, 3)), pltpu.SemaphoreType.DMA((tiles, 4, 3))]


def scatter_scratch(slots):
    return ([pltpu.VMEM((slots, 3, D, FT), BF)] + [pltpu.VMEM((slots, 3, n, FT), BF) for n in HALVES]
            + [pltpu.VMEM((slots, 3, n, FT), BF) for n in HALVES[1:]]
            + [pltpu.SemaphoreType.DMA((4, 3, slots)), pltpu.SemaphoreType.DMA((4, 3, slots))])


def scatter_of(refs):
    return Scatter(refs[0], refs[1:5], refs[5:8], refs[8], refs[9])


EARLY = 3


def kernel_b(h_hbm, dy_hbm, wg_ref, wu_ref, wd_ref, full_hbm, late_hbm, squares_ref, dh_hbm, dht_hbm,
             a_ref, dy_ref, at_ref, dt_ref, accg_ref, accu_ref, hid_ref, dg_ref, du_ref, sem, shard_ref, *rest):
    t = pl.program_id(0)
    s = scatter_of(rest[:10])
    g = Gather(shard_ref, full_hbm, *rest[10:])
    store_late = pltpu.make_async_copy(shard_ref.at[pl.ds(EARLY, NT - EARLY)], late_hbm, sem.at[4])
    load_h = pltpu.make_async_copy(h_hbm, a_ref, sem.at[0])
    load_dy = pltpu.make_async_copy(dy_hbm, dy_ref, sem.at[1])
    store_dh = pltpu.make_async_copy(dy_ref, dh_hbm, sem.at[2])
    store_dht = pltpu.make_async_copy(dt_ref, dht_hbm, sem.at[3])
    now, before = t % 2, (t + 1) % 2

    @pl.when(t == 0)
    def _():
        load_h.start()
        load_dy.start()
        greet()
        squares_ref[...] = jnp.zeros_like(squares_ref)
        load_h.wait()
        norm_into(a_ref, a_ref, at_ref)
        load_dy.wait()
        transpose_into(dy_ref, dt_ref)

    def body(first, i, _):
        r = rows(i, MB)
        a = a_ref[r, :]
        gate = dot(a, wg_ref[0])
        up = dot(a, wu_ref[0])
        dhid = dot(dy_ref[r, :], wd_ref[0], NTR)
        hid, dg, du = back_elementwise(gate, up, dhid)
        hid_ref[r, :] = hid
        dg_ref[r, :] = dg
        du_ref[r, :] = du
        yg = dot(dg, wg_ref[0], NTR)
        yu = dot(du, wu_ref[0], NTR)
        if first:
            accg_ref[r, :] = yg
            accu_ref[r, :] = yu
        else:
            accg_ref[r, :] += yg
            accu_ref[r, :] += yu
        return 0

    def half(lo):
        @pl.when(t == 0)
        def _():
            lax.fori_loop(lo, lo + 2, functools.partial(body, True), 0)

        @pl.when((t > 0) & (t < NT))
        def _():
            lax.fori_loop(lo, lo + 2, functools.partial(body, False), 0)

    def advance(stage):
        @pl.when(t > 0)
        def _():
            s.advance(before, stage)

    def grads(lo):
        @pl.when(t < NT)
        def _():
            weight_grads(at_ref, dt_ref, hid_ref, dg_ref, du_ref, s.g, now, lo, lo + 2)

    def collect(stage, behind):
        @pl.when((t >= behind) & (t < behind + EARLY))
        def _():
            if stage == 4:
                g.finish(t - behind)
            else:
                g.advance(t - behind, stage)

    half(0)
    collect(3, 3)
    advance(1)
    collect(1, 2)
    half(2)

    @pl.when(t == NT - 1)
    def _():
        load_h.start()

    advance(2)
    grads(0)

    @pl.when(t == NT)
    def _():
        load_h.wait()

        def fin(i, _):
            r = rows(i, 256)
            wide = a_ref[r, :].astype(F32)
            scale = lax.rsqrt(jnp.mean(wide * wide, -1, keepdims=True) + 1e-6)
            da = (accg_ref[r, :].astype(BF).astype(F32) + accu_ref[r, :].astype(BF).astype(F32)).astype(BF).astype(F32)
            inner = jnp.mean(da * wide, -1, keepdims=True)
            dn = (da * scale - wide * (scale * scale * scale * inner)).astype(BF).astype(F32)
            dh = (dy_ref[r, :].astype(F32) + dn).astype(BF)
            dy_ref[r, :] = dh
            dt_ref[:, r] = dh.T
            return 0
        lax.fori_loop(0, T // 256, fin, 0)
        store_dh.start()
        store_dht.start()

    advance(3)
    collect(2, 2)
    collect(4, 3)
    grads(2)

    @pl.when(t > 0)
    def _():
        s.finish(before, shard_ref.at[jnp.maximum(t - 1, 0)], squares_ref)

    @pl.when((t >= 1) & (t < 1 + EARLY))
    def _():
        g.begin(t - 1)

    @pl.when(t < NT)
    def _():
        s.begin(now)

    @pl.when(t == NT)
    def _():
        store_late.start()
        store_dh.wait()
        store_dht.wait()
        store_late.wait()


def layer1(h1, dy, wg, wu, wd):
    any_ = pl.BlockSpec(memory_space=pl.ANY)
    at = lambda t: jnp.minimum(t, NT - 1)
    return pl.pallas_call(
        kernel_b,
        grid=(NT + 1,),
        in_specs=[any_, any_,
                  pl.BlockSpec((1, D, FT), lambda t: (1, 0, at(t))),
                  pl.BlockSpec((1, D, FT), lambda t: (1, 0, at(t))),
                  pl.BlockSpec((1, FT, D), lambda t: (1, at(t), 0))],
        out_specs=[any_, any_, pl.BlockSpec((8, 128), lambda t: (0, 0)), any_, any_],
        out_shape=[jax.ShapeDtypeStruct((3, D, EARLY * FT), BF), jax.ShapeDtypeStruct((NT - EARLY, 3, 64, FT), BF),
                   jax.ShapeDtypeStruct((8, 128), F32), jax.ShapeDtypeStruct((T, D), BF), jax.ShapeDtypeStruct((D, T), BF)],
        scratch_shapes=[pltpu.VMEM((T, D), BF), pltpu.VMEM((T, D), BF), pltpu.VMEM((D, T), BF), pltpu.VMEM((D, T), BF),
                        pltpu.VMEM((T, D), F32), pltpu.VMEM((T, D), F32),
                        pltpu.VMEM((T, FT), BF), pltpu.VMEM((T, FT), BF), pltpu.VMEM((T, FT), BF), pltpu.SemaphoreType.DMA((5,)),
                        pltpu.VMEM((NT, 3, 64, FT), BF)]
        + scatter_scratch(2) + gather_scratch(EARLY),
        compiler_params=params(collective_id=1, has_side_effects=True),
        cost_estimate=pl.CostEstimate(flops=16 * T * D * F, bytes_accessed=12 * D * F + 6 * T * D, transcendentals=0),
        name="layer1",
    )(h1, dy, wg, wu, wd)


def kernel_c(at_ref, dh_ref, dt_ref, gate_ref, up_ref, wd_ref, late_ref, squares1_ref, shard_ref, full_hbm, factor_ref,
             hid_ref, dg_ref, du_ref, squares_ref, xs, xr, x_send, x_recv, *rest):
    t = pl.program_id(0)
    s = scatter_of(rest[:10])
    gat = Gather(late_ref, full_hbm, *rest[10:])

    def collect(step, stage):
        @pl.when(t == step)
        def _():
            for tile in range(NT - EARLY):
                if stage == 0:
                    gat.begin(tile)
                elif stage == 4:
                    gat.finish(tile)
                else:
                    gat.advance(tile, stage)

    now, one, two = t % 3, (t + 2) % 3, (t + 1) % 3

    @pl.when(t == 0)
    def _():
        greet()
        squares_ref[...] = squares1_ref[...]

    collect(0, 0)

    @pl.when(t < NT)
    def _():
        def body(i, _):
            r = rows(i, MB)
            dhid = dot(dh_ref[r, :], wd_ref[0], NTR)
            hid, dg, du = back_elementwise(gate_ref[r, :], up_ref[r, :], dhid)
            hid_ref[r, :] = hid
            dg_ref[r, :] = dg
            du_ref[r, :] = du
            return 0
        lax.fori_loop(0, T // MB, body, 0)

    def grads(lo):
        @pl.when(t < NT)
        def _():
            weight_grads(at_ref, dt_ref, hid_ref, dg_ref, du_ref, s.g, now, lo, lo + 2)

    @pl.when(t >= 2)
    def _():
        s.advance(two, 3)

    @pl.when((t >= 1) & (t <= NT))
    def _():
        s.advance(one, 1)

    collect(0, 1)
    collect(2, 4)
    grads(0)

    @pl.when(t >= 2)
    def _():
        s.finish(two, shard_ref, squares_ref)

    collect(0, 2)
    collect(1, 3)
    grads(2)

    @pl.when(t < NT)
    def _():
        s.begin(now)

    @pl.when((t >= 1) & (t <= NT))
    def _():
        s.advance(one, 2)

    @pl.when(t == NT + 1)
    def _():
        total = squares_ref[...]
        for k, stride in enumerate(PARTNERS):
            xs[k] = total
            copy = pltpu.make_async_remote_copy(src_ref=xs.at[k], dst_ref=xr.at[k], send_sem=x_send.at[k], recv_sem=x_recv.at[k],
                                                device_id=partner(stride), device_id_type=pl.DeviceIdType.MESH)
            copy.start()
            copy.wait()
            total = total + xr[k]
        total = jnp.sum(jnp.sum(total, 0, keepdims=True), 1, keepdims=True)
        factor_ref[...] = jnp.broadcast_to(jnp.minimum(1.0, 0.5 * lax.rsqrt(total / (6 * D * F) + 1e-30)), (8, 128))


def back0(at0, dh1, dht1, gate, up, wd, late, squares1):
    whole = pl.BlockSpec((T, D), lambda t: (0, 0), pipeline_mode=pl.Buffered(1))
    turned = pl.BlockSpec((D, T), lambda t: (0, 0), pipeline_mode=pl.Buffered(1))
    at = lambda t: jnp.minimum(t, NT - 1)
    return pl.pallas_call(
        kernel_c,
        grid=(NT + 2,),
        in_specs=[turned, whole, turned, pl.BlockSpec((T, FT), lambda t: (0, at(t))), pl.BlockSpec((T, FT), lambda t: (0, at(t))),
                  pl.BlockSpec((1, FT, D), lambda t: (0, at(t), 0)),
                  pl.BlockSpec((NT - EARLY, 3, 64, FT), lambda t: (0, 0, 0, 0)), pl.BlockSpec((8, 128), lambda t: (0, 0))],
        out_specs=[pl.BlockSpec((3, 64, FT), lambda t: (0, 0, jnp.maximum(t - 2, 0))), pl.BlockSpec(memory_space=pl.ANY),
                   pl.BlockSpec((8, 128), lambda t: (0, 0))],
        out_shape=[jax.ShapeDtypeStruct((3, 64, F), BF), jax.ShapeDtypeStruct((3, D, (NT - EARLY) * FT), BF), jax.ShapeDtypeStruct((8, 128), F32)],
        scratch_shapes=[pltpu.VMEM((T, FT), BF), pltpu.VMEM((T, FT), BF), pltpu.VMEM((T, FT), BF), pltpu.VMEM((8, 128), F32),
                        pltpu.VMEM((4, 8, 128), F32), pltpu.VMEM((4, 8, 128), F32), pltpu.SemaphoreType.DMA((4,)), pltpu.SemaphoreType.DMA((4,))]
        + scatter_scratch(3) + gather_scratch(NT - EARLY),
        compiler_params=params(collective_id=2, has_side_effects=True),
        cost_estimate=pl.CostEstimate(flops=8 * T * D * F, bytes_accessed=8 * T * F + 8 * D * F, transcendentals=0),
        name="back0",
    )(at0, dh1, dht1, gate, up, wd, late, squares1)


FB = 256


def adamw(w, m, v, g):
    m = 0.9 * m + 0.1 * g
    v = 0.95 * v + 0.05 * g * g
    w = w.astype(F32)
    return (w - 0.02 * (m * lax.rsqrt(v + 1e-8) + 0.1 * w)).astype(BF), m, v


def update(refs, outs, i, where, g):
    at = (0,) + where
    new = adamw(refs[i][at], refs[3 + i][at], refs[6 + i][at], g)
    for k in range(3):
        outs[3 * k + i][at] = new[k]


def kernel_o1(f_ref, early_ref, late_ref, *refs):
    ins, outs = refs[:9], refs[-9:]
    factor = f_ref[0:1, 0:1]

    def run(g_ref):
        for i in range(3):
            g = g_ref[i].astype(F32)
            update(ins, outs, i, (slice(None), slice(None)), (g.T if i == 2 else g) * factor)

    early = EARLY * FT // FB

    @pl.when(pl.program_id(0) < early)
    def _():
        run(early_ref)

    @pl.when(pl.program_id(0) >= early)
    def _():
        run(late_ref)


def owner(c, k):
    return sum(s * (k * 64 // HALVES[i] % 2) for i, s in enumerate(strides(c)))


def kernel_o0(f_ref, g_ref, *refs):
    ins, outs = refs[:9], refs[-9:]
    factor = f_ref[0:1, 0:1]
    for k in range(8):
        both = slice(128 * k, 128 * k + 128)
        for i in range(3):
            g = jnp.concatenate([g_ref[owner(i, 2 * k + half), i] for half in range(2)], 0).astype(F32)
            where = (slice(None), both) if i == 2 else (both, slice(None))
            update(ins, outs, i, where, (g.T if i == 2 else g) * factor)


def optimizer(layer, kernel, factor, gradients, specs, arrays, before):
    wide = pl.BlockSpec((1, D, FB), lambda t: (layer, 0, t))
    tall = pl.BlockSpec((1, FB, D), lambda t: (layer, t, 0))
    three = [wide, wide, tall]
    first = 1 + len(gradients) + 9
    return pl.pallas_call(
        kernel,
        grid=(F // FB,),
        in_specs=[pl.BlockSpec((8, 128), lambda t: (0, 0))] + specs + three * 3 + [pl.BlockSpec(memory_space=pl.ANY)] * len(before),
        out_specs=three * 3,
        out_shape=[jax.ShapeDtypeStruct(a.shape, a.dtype) for a in arrays],
        input_output_aliases={first + i: i for i in range(len(before))},
        compiler_params=params(),
        cost_estimate=pl.CostEstimate(flops=30 * D * F, bytes_accessed=66 * D * F, transcendentals=3 * D * F),
        name=f"adamw{layer}",
    )(factor, *gradients, *arrays, *before)


def solution(mesh):
    def step(x, dy, *arrays):
        wg, wu, wd = arrays[:3]
        gate, up, h1, at0 = forward0(x[0], wg, wu, wd)
        early, late, squares1, dh1, dht1 = layer1(h1, dy[0], wg, wu, wd)
        s0, rest, factor = back0(at0, dh1, dht1, gate, up, wd, late, squares1)
        full0 = lax.all_gather(s0, "dp")
        n = EARLY * FT // FB
        specs = [pl.BlockSpec((3, D, FB), lambda t: (0, 0, jnp.minimum(t, n - 1))),
                 pl.BlockSpec((3, D, FB), lambda t: (0, 0, jnp.maximum(t - n, 0)))]
        new = optimizer(1, kernel_o1, factor, (early, rest), specs, arrays, ())
        specs = [pl.BlockSpec((16, 3, 64, FB), lambda t: (0, 0, 0, t))]
        return tuple(optimizer(0, kernel_o0, factor, (full0,), specs, arrays, new))

    return jax.shard_map(
        step,
        mesh=mesh,
        in_specs=(P(("rep", "dp"), None, None),) * 2 + (P(None, None, None),) * 9,
        out_specs=(P("rep", None, None),) * 9,
        check_vma=False,
    )
```

```python
import functools
import jax
import jax.numpy as jnp
from jax import lax
from jax.experimental import pallas as pl
from jax.experimental.pallas import tpu as pltpu
from jax.sharding import PartitionSpec as P

T, D, F = 2048, 1024, 2560
FT = 512
NT = F // FT
MB = 512
BF, F32 = jnp.bfloat16, jnp.float32
VL = 64 * 1024 * 1024 - 128 * 1024
NN = (((1,), (0,)), ((), ()))
NTR = (((1,), (1,)), ((), ()))
TN = (((0,), (0,)), ((), ()))


def dot(a, b, dims=NN):
    return lax.dot_general(a, b, dims, preferred_element_type=F32)


def params(**more):
    return pltpu.CompilerParams(vmem_limit_bytes=VL, dimension_semantics=("arbitrary",), **more)


def norm_block(h):
    wide = h.astype(F32)
    scale = lax.rsqrt(jnp.mean(wide * wide, -1, keepdims=True) + 1e-6)
    return (wide * scale).astype(BF)


def rows(i, n):
    return pl.ds(pl.multiple_of(i * n, n), n)


def norm_into(h_ref, a_ref, n=256):
    def body(i, _):
        a_ref[rows(i, n), :] = norm_block(h_ref[rows(i, n), :])
        return 0
    lax.fori_loop(0, T // n, body, 0)


def kernel_a(x_ref, wg_ref, wu_ref, wd_ref, gate_ref, up_ref, h1_ref, a_ref, acc_ref):
    t = pl.program_id(0)

    @pl.when(t == 0)
    def _():
        norm_into(x_ref, a_ref)

    def body(first, i, _):
        r = rows(i, MB)
        a = a_ref[r, :]
        gate = dot(a, wg_ref[0])
        up = dot(a, wu_ref[0])
        gate_ref[r, :] = gate
        up_ref[r, :] = up
        hid = (gate * jax.nn.sigmoid(gate) * up).astype(BF)
        y = dot(hid, wd_ref[0])
        if first:
            acc_ref[r, :] = y
        else:
            acc_ref[r, :] += y
        return 0

    @pl.when(t == 0)
    def _():
        lax.fori_loop(0, T // MB, functools.partial(body, True), 0, unroll=2)

    @pl.when(t > 0)
    def _():
        lax.fori_loop(0, T // MB, functools.partial(body, False), 0, unroll=2)

    @pl.when(t == NT - 1)
    def _():
        def fin(i, _):
            r = rows(i, MB)
            h1_ref[r, :] = (x_ref[r, :].astype(F32) + acc_ref[r, :].astype(BF).astype(F32)).astype(BF)
            return 0
        lax.fori_loop(0, T // MB, fin, 0)


def forward0(x, wg, wu, wd):
    whole = pl.BlockSpec((T, D), lambda t: (0, 0), pipeline_mode=pl.Buffered(1))
    return pl.pallas_call(
        kernel_a,
        grid=(NT,),
        in_specs=[whole,
                  pl.BlockSpec((1, D, FT), lambda t: (0, 0, t)),
                  pl.BlockSpec((1, D, FT), lambda t: (0, 0, t)),
                  pl.BlockSpec((1, FT, D), lambda t: (0, t, 0))],
        out_specs=[pl.BlockSpec((T, FT), lambda t: (0, t)), pl.BlockSpec((T, FT), lambda t: (0, t)), whole, whole],
        out_shape=[jax.ShapeDtypeStruct((T, F), F32), jax.ShapeDtypeStruct((T, F), F32), jax.ShapeDtypeStruct((T, D), BF),
                   jax.ShapeDtypeStruct((T, D), BF)],
        scratch_shapes=[pltpu.VMEM((T, D), F32)],
        compiler_params=params(),
        cost_estimate=pl.CostEstimate(flops=6 * T * D * F, bytes_accessed=8 * T * F + 6 * D * F, transcendentals=0),
        name="fwd0",
    )(x, wg, wu, wd)


def back_elementwise(gate, up, dhid):
    s = jax.nn.sigmoid(gate)
    silu = gate * s
    dh = dhid.astype(BF).astype(F32)
    hid = (silu * up).astype(BF)
    du = (dh * silu).astype(BF)
    dg = (dh * up * (s + silu * (1.0 - s))).astype(BF)
    return hid, dg, du


def weight_grads(a_ref, d_ref, hid_ref, dg_ref, du_ref, g_ref, slot, n):
    r = rows(n, 512)
    g_ref[slot, 0, r, :] = dot(a_ref[:, r], dg_ref[...], TN).astype(BF)
    g_ref[slot, 1, r, :] = dot(a_ref[:, r], du_ref[...], TN).astype(BF)
    g_ref[slot, 2, r, :] = dot(d_ref[:, r], hid_ref[...], TN).astype(BF)


CORE = 1
ORDER = ((8, 4, 2), (4, 2, 8), (2, 8, 4))
PARTNERS = (1, 2, 4, 8)
HALVES = (512, 256, 128, 64)


def bit(stride):
    return (lax.axis_index("dp") // stride) % 2


def partner(stride):
    return {"dp": lax.axis_index("dp") + stride * (1 - 2 * bit(stride))}


def across(k):
    return {"dp": lax.axis_index("dp") + sum(stride * (1 - 2 * bit(stride)) for stride in PARTNERS if k & stride)}


def greet(devices):
    barrier = pltpu.get_barrier_semaphore()
    for device in devices:
        pl.semaphore_signal(barrier, inc=1, device_id=device, device_id_type=pl.DeviceIdType.MESH)
    pl.semaphore_wait(barrier, len(devices))


def some(start, n):
    return pl.ds(pl.multiple_of(start, 64), n)


def strides(c):
    return (CORE,) + ORDER[c]


class Scatter:
    def __init__(self, g, got, sent, send_sem, recv_sem):
        self.g, self.got, self.sent, self.send_sem, self.recv_sem = g, got, sent, send_sem, recv_sem

    def total(self, tile, c, keep):
        def read(ref, first):
            start = sum(b * HALVES[i] for i, b in enumerate(keep) if i >= first)
            return ref[tile % ref.shape[0], c, some(start, HALVES[len(keep) - 1]), :].astype(F32)
        out = read(self.g, 0)
        for stage in range(min(4, len(keep) if self.whole else len(keep) - 1)):
            out = out + read(self.got[stage], stage + 1)
        return out

    def copy(self, tile, c, stage):
        if stage == 0:
            src = self.g.at[tile % self.g.shape[0], c, some((1 - bit(CORE)) * 512, 512), :]
        else:
            src = self.sent[stage - 1].at[tile % self.sent[stage - 1].shape[0], c]
        got = self.got[stage]
        return pltpu.make_async_remote_copy(
            src_ref=src, dst_ref=got.at[tile % got.shape[0], c], send_sem=self.send_sem.at[stage, c, tile % 3], recv_sem=self.recv_sem.at[stage, c, tile % 3],
            device_id=partner(strides(c)[stage]), device_id_type=pl.DeviceIdType.MESH)

    def begin(self, tile):
        for c in range(3):
            self.copy(tile, c, 0).start()

    def advance(self, tile, stage):
        self.whole = False
        for c in range(3):
            self.copy(tile, c, stage - 1).wait_recv()
            if stage == 3:
                self.copy(tile, c, 1).wait_send()
            bits = [bit(s) for s in strides(c)]
            sent = self.sent[stage - 1]
            sent[tile % sent.shape[0], c] = self.total(tile, c, bits[:stage] + [1 - bits[stage]]).astype(BF)
            self.copy(tile, c, stage).start()

    def finish(self, tile, put, squares_ref):
        self.whole = True
        for c in range(3):
            self.copy(tile, c, 3).wait_recv()
            out = self.total(tile, c, [bit(s) for s in strides(c)]).astype(BF)
            put(c, out)
            squares = out.astype(F32) * out.astype(F32)
            squares_ref[...] += sum(squares[8 * i:8 * i + 8, 128 * j:128 * j + 128] for i in range(8) for j in range(FT // 128))
            for stage in (0, 2, 3):
                self.copy(tile, c, stage).wait_send()


class Gather:
    def __init__(self, full, hbm, own_sem, send_sem, recv_sem):
        self.full, self.hbm, self.own_sem, self.send_sem, self.recv_sem = full, hbm, own_sem, send_sem, recv_sem

    def place(self, tile, c, n):
        start = sum(bit(s) * HALVES[i] for i, s in enumerate(strides(c)) if HALVES[i] >= n)
        return self.full.at[tile, c, some(start, n), :]

    def put(self, tile):
        def store(c, out):
            self.place(tile, c, 64)[...] = out
        return store

    def copy(self, tile, c, stage):
        place = self.place(tile, c, 64 << stage)
        return pltpu.make_async_remote_copy(
            src_ref=place, dst_ref=place, send_sem=self.send_sem.at[tile, stage, c], recv_sem=self.recv_sem.at[tile, stage, c],
            device_id=partner(strides(c)[3 - stage]), device_id_type=pl.DeviceIdType.MESH)

    def store(self, tile):
        return pltpu.make_async_copy(self.full.at[tile], self.hbm.at[tile], self.own_sem.at[tile])

    def begin(self, tile):
        for c in range(3):
            self.copy(tile, c, 0).start()

    def advance(self, tile, stage):
        for c in range(3):
            self.copy(tile, c, stage - 1).wait_recv()
            self.copy(tile, c, stage).start()

    def finish(self, tile):
        for c in range(3):
            self.copy(tile, c, 3).wait_recv()
            for stage in range(4):
                self.copy(tile, c, stage).wait_send()
        self.store(tile).start()


def gather_scratch(tiles):
    return [pltpu.VMEM((tiles, 3, D, FT), BF), pltpu.SemaphoreType.DMA((tiles,)), pltpu.SemaphoreType.DMA((tiles, 4, 3)),
            pltpu.SemaphoreType.DMA((tiles, 4, 3))]


def scatter_scratch(slots, got_slots, sent_slots):
    return ([pltpu.VMEM((slots, 3, D, FT), BF)] + [pltpu.VMEM((k, 3, n, FT), BF) for k, n in zip(got_slots, HALVES, strict=True)]
            + [pltpu.VMEM((k, 3, n, FT), BF) for k, n in zip(sent_slots, HALVES[1:], strict=True)]
            + [pltpu.SemaphoreType.DMA((4, 3, 3)), pltpu.SemaphoreType.DMA((4, 3, 3))])


def scatter_of(refs):
    return Scatter(refs[0], refs[1:5], refs[5:8], refs[8], refs[9])


EARLY = 2


def kernel_b(h_hbm, dy_hbm, wg_ref, wu_ref, wd_ref, full_hbm, late_hbm, squares_ref, dh_hbm,
             a_ref, dy_ref, accg_ref, accu_ref, hid_ref, dg_ref, du_ref, sem, shard_ref, *rest):
    t = pl.program_id(0)
    s = scatter_of(rest[:10])
    g = Gather(rest[10], full_hbm, *rest[11:])
    store_late = pltpu.make_async_copy(shard_ref, late_hbm, sem.at[3])
    load_h = pltpu.make_async_copy(h_hbm, a_ref, sem.at[0])
    load_dy = pltpu.make_async_copy(dy_hbm, dy_ref, sem.at[1])
    store_dh = pltpu.make_async_copy(dy_ref, dh_hbm, sem.at[2])

    @pl.when(t == 0)
    def _():
        load_h.start()
        load_dy.start()
        greet([partner(stride) for stride in PARTNERS])
        squares_ref[...] = jnp.zeros_like(squares_ref)

        def clear(i, _):
            accg_ref[rows(i, 64), :] = jnp.zeros((64, D), F32)
            accu_ref[rows(i, 64), :] = jnp.zeros((64, D), F32)
            return 0
        lax.fori_loop(0, T // 64, clear, 0)
        load_h.wait()
        norm_into(a_ref, a_ref)
        load_dy.wait()

    def body(i):
        r = rows(i, MB)
        a = a_ref[r, :]
        gate = dot(a, wg_ref[0])
        up = dot(a, wu_ref[0])
        dhid = dot(dy_ref[r, :], wd_ref[0], NTR)
        hid, dg, du = back_elementwise(gate, up, dhid)
        hid_ref[r, :] = hid
        dg_ref[r, :] = dg
        du_ref[r, :] = du
        yg = dot(dg, wg_ref[0], NTR)
        yu = dot(du, wu_ref[0], NTR)
        accg_ref[r, :] += yg
        accu_ref[r, :] += yu

    def behind(steps, do, last=NT, first=0):
        @pl.when((t >= steps + first) & (t < steps + last) & (t < NT))
        def _():
            do(t - steps)

    def early(tile):
        s.finish(tile, g.put(tile), squares_ref)
        g.begin(tile)

    def late(tile):
        def put(c, out):
            shard_ref[tile - EARLY, c] = out
        s.finish(tile, put, squares_ref)

    def first_loop(i, _):
        body(i)

        @pl.when(i == 1)
        def _():
            behind(2, lambda tile: s.advance(tile, 3))
            behind(1, lambda tile: s.advance(tile, 1))
            behind(3, lambda tile: g.advance(tile, 2), EARLY)
        return 0

    def second_loop(n, _):
        weight_grads(a_ref, dy_ref, hid_ref, dg_ref, du_ref, s.g, t % 2, n)

        @pl.when(n == 0)
        def _():
            behind(1, lambda tile: s.advance(tile, 2))
            behind(3, lambda tile: g.advance(tile, 3), EARLY)
        return 0

    @pl.when(t < NT)
    def _():
        lax.fori_loop(0, T // MB, first_loop, 0)
        behind(2, early, EARLY)
        behind(2, late, NT, EARLY)
        behind(4, g.finish, EARLY)
        lax.fori_loop(0, D // 512, second_loop, 0)
        behind(0, s.begin)
        behind(2, lambda tile: g.advance(tile, 1), EARLY)

    @pl.when(t == NT)
    def _():
        load_h.start()
        s.advance(NT - 2, 3)
        s.advance(NT - 1, 1)
        load_h.wait()

        def fin(i, _):
            r = rows(i, 256)
            wide = a_ref[r, :].astype(F32)
            scale = lax.rsqrt(jnp.mean(wide * wide, -1, keepdims=True) + 1e-6)
            da = (accg_ref[r, :].astype(BF).astype(F32) + accu_ref[r, :].astype(BF).astype(F32)).astype(BF).astype(F32)
            inner = jnp.mean(da * wide, -1, keepdims=True)
            dn = (da * scale - wide * (scale * scale * scale * inner)).astype(BF).astype(F32)
            dh = (dy_ref[r, :].astype(F32) + dn).astype(BF)
            dy_ref[r, :] = dh
            return 0
        lax.fori_loop(0, T // 256, fin, 0)
        store_dh.start()
        s.advance(NT - 1, 2)
        late(NT - 2)
        g.finish(NT - 4)
        s.advance(NT - 1, 3)
        late(NT - 1)
        store_late.start()
        store_dh.wait()
        for tile in range(EARLY):
            g.store(tile).wait()
        store_late.wait()


def layer1(h1, dy, wg, wu, wd):
    any_ = pl.BlockSpec(memory_space=pl.ANY)
    at = lambda t: jnp.minimum(t, NT - 1)
    return pl.pallas_call(
        kernel_b,
        grid=(NT + 1,),
        in_specs=[any_, any_,
                  pl.BlockSpec((1, D, FT), lambda t: (1, 0, at(t))),
                  pl.BlockSpec((1, D, FT), lambda t: (1, 0, at(t))),
                  pl.BlockSpec((1, FT, D), lambda t: (1, at(t), 0))],
        out_specs=[any_, any_, pl.BlockSpec((8, 128), lambda t: (0, 0)), any_],
        out_shape=[jax.ShapeDtypeStruct((EARLY, 3, D, FT), BF), jax.ShapeDtypeStruct((NT - EARLY, 3, 64, FT), BF),
                   jax.ShapeDtypeStruct((8, 128), F32), jax.ShapeDtypeStruct((T, D), BF)],
        scratch_shapes=[pltpu.VMEM((T, D), BF), pltpu.VMEM((T, D), BF),
                        pltpu.VMEM((T, D), F32), pltpu.VMEM((T, D), F32),
                        pltpu.VMEM((T, FT), BF), pltpu.VMEM((T, FT), BF), pltpu.VMEM((T, FT), BF), pltpu.SemaphoreType.DMA((4,)),
                        pltpu.VMEM((NT - EARLY, 3, 64, FT), BF)]
        + scatter_scratch(2, (3, 3, 2, 2), (1, 2, 2)) + gather_scratch(EARLY),
        compiler_params=params(collective_id=1, has_side_effects=True),
        cost_estimate=pl.CostEstimate(flops=16 * T * D * F, bytes_accessed=12 * D * F + 6 * T * D, transcendentals=0),
        name="layer1",
    )(h1, dy, wg, wu, wd)


def kernel_c(a_hbm, dh_ref, gate_ref, up_ref, wd_ref, squares1_ref, shard_ref, factor_ref,
             a_ref, sem, hid_ref, dg_ref, du_ref, squares_ref, xs, xr, x_send, x_recv, *rest):
    t = pl.program_id(0)
    s = scatter_of(rest)
    load_a = pltpu.make_async_copy(a_hbm, a_ref, sem.at[0])

    def put(c, out):
        shard_ref[c] = out

    def behind(steps, do):
        @pl.when((t >= steps) & (t < steps + NT))
        def _():
            do(t - steps)

    @pl.when(t == 0)
    def _():
        load_a.start()
        greet([across(k) for k in range(1, 16)])
        squares_ref[...] = squares1_ref[...]

    @pl.when(t < NT)
    def _():
        def body(i, _):
            r = rows(i, MB)
            dhid = dot(dh_ref[r, :], wd_ref[0], NTR)
            hid, dg, du = back_elementwise(gate_ref[r, :], up_ref[r, :], dhid)
            hid_ref[r, :] = hid
            dg_ref[r, :] = dg
            du_ref[r, :] = du
            return 0
        lax.fori_loop(0, T // MB, body, 0)

    @pl.when(t == 0)
    def _():
        load_a.wait()

    behind(1, lambda tile: s.advance(tile, 1))
    def loop(n, _):
        @pl.when(t < NT)
        def _():
            weight_grads(a_ref, dh_ref, hid_ref, dg_ref, du_ref, s.g, t % 3, n)

        @pl.when(n == 0)
        def _():
            behind(2, lambda tile: s.advance(tile, 3))
        return 0
    lax.fori_loop(0, D // 512, loop, 0)
    behind(2, lambda tile: s.finish(tile, put, squares_ref))
    behind(0, s.begin)
    behind(1, lambda tile: s.advance(tile, 2))

    @pl.when(t == NT + 1)
    def _():
        xs[...] = squares_ref[...]
        copies = [pltpu.make_async_remote_copy(src_ref=xs, dst_ref=xr.at[k], send_sem=x_send.at[k], recv_sem=x_recv.at[k],
                                               device_id=across(k), device_id_type=pl.DeviceIdType.MESH) for k in range(1, 16)]
        for copy in copies:
            copy.start()
        for copy in copies:
            copy.wait()
        terms = [squares_ref[...]] + [xr[k] for k in range(1, 16)]
        while len(terms) > 1:
            terms = [one + two for one, two in zip(terms[::2], terms[1::2], strict=True)]
        total = terms[0]
        total = jnp.sum(jnp.sum(total, 0, keepdims=True), 1, keepdims=True)
        factor_ref[...] = jnp.broadcast_to(jnp.minimum(1.0, 0.5 * lax.rsqrt(total / (6 * D * F) + 1e-30)), (8, 128))


def back0(a0, dh1, gate, up, wd, squares1):
    whole = pl.BlockSpec((T, D), lambda t: (0, 0), pipeline_mode=pl.Buffered(1))
    any_ = pl.BlockSpec(memory_space=pl.ANY)
    at = lambda t: jnp.minimum(t, NT - 1)
    return pl.pallas_call(
        kernel_c,
        grid=(NT + 2,),
        in_specs=[any_, whole, pl.BlockSpec((T, FT), lambda t: (0, at(t))), pl.BlockSpec((T, FT), lambda t: (0, at(t))),
                  pl.BlockSpec((1, FT, D), lambda t: (0, at(t), 0)),
                  pl.BlockSpec((8, 128), lambda t: (0, 0))],
        out_specs=[pl.BlockSpec((3, 64, FT), lambda t: (0, 0, jnp.maximum(t - 2, 0))),
                   pl.BlockSpec((8, 128), lambda t: (0, 0))],
        out_shape=[jax.ShapeDtypeStruct((3, 64, F), BF), jax.ShapeDtypeStruct((8, 128), F32)],
        scratch_shapes=[pltpu.VMEM((T, D), BF), pltpu.SemaphoreType.DMA((1,)),
                        pltpu.VMEM((T, FT), BF), pltpu.VMEM((T, FT), BF), pltpu.VMEM((T, FT), BF), pltpu.VMEM((8, 128), F32),
                        pltpu.VMEM((8, 128), F32), pltpu.VMEM((16, 8, 128), F32), pltpu.SemaphoreType.DMA((16,)), pltpu.SemaphoreType.DMA((16,))]
        + scatter_scratch(3, (3, 3, 3, 3), (3, 3, 3)),
        compiler_params=params(collective_id=2, has_side_effects=True),
        cost_estimate=pl.CostEstimate(flops=8 * T * D * F, bytes_accessed=8 * T * F + 8 * D * F, transcendentals=0),
        name="back0",
    )(a0, dh1, gate, up, wd, squares1)


FB = 256


def adamw(w, m, v, g):
    m = 0.9 * m + 0.1 * g
    v = 0.95 * v + 0.05 * g * g
    w = w.astype(F32)
    return (w - 0.02 * (m * lax.rsqrt(v + 1e-8) + 0.1 * w)).astype(BF), m, v


def update(refs, outs, i, where, g):
    at = (0,) + where
    new = adamw(refs[i][at], refs[3 + i][at], refs[6 + i][at], g)
    for k in range(3):
        outs[3 * k + i][at] = new[k]


def owner(c, k):
    return sum(s * (k * 64 // HALVES[i] % 2) for i, s in enumerate(strides(c)))


def update_all(refs, outs, factor, gathered):
    for k in range(8):
        both = slice(128 * k, 128 * k + 128)
        for i in range(3):
            g = jnp.concatenate([gathered(owner(i, 2 * k + half), i) for half in range(2)], 0).astype(F32)
            where = (slice(None), both) if i == 2 else (both, slice(None))
            update(refs, outs, i, where, (g.T if i == 2 else g) * factor)


def kernel_o1(f_ref, early_ref, late_ref, *refs):
    ins, outs = refs[:9], refs[-9:]
    factor = f_ref[0:1, 0:1]
    early = EARLY * FT // FB

    @pl.when(pl.program_id(0) < early)
    def _():
        for i in range(3):
            g = early_ref[0, i].astype(F32)
            update(ins, outs, i, (slice(None), slice(None)), (g.T if i == 2 else g) * factor)

    @pl.when(pl.program_id(0) >= early)
    def _():
        update_all(ins, outs, factor, lambda device, i: late_ref[device, 0, i])


def kernel_o0(f_ref, g_ref, *refs):
    update_all(refs[:9], refs[-9:], f_ref[0:1, 0:1], lambda device, i: g_ref[device, i])


def optimizer(layer, kernel, factor, gradients, specs, arrays, before):
    wide = pl.BlockSpec((1, D, FB), lambda t: (layer, 0, t))
    tall = pl.BlockSpec((1, FB, D), lambda t: (layer, t, 0))
    three = [wide, wide, tall]
    first = 1 + len(gradients) + 9
    return pl.pallas_call(
        kernel,
        grid=(F // FB,),
        in_specs=[pl.BlockSpec((8, 128), lambda t: (0, 0))] + specs + three * 3 + [pl.BlockSpec(memory_space=pl.ANY)] * len(before),
        out_specs=three * 3,
        out_shape=[jax.ShapeDtypeStruct(a.shape, a.dtype) for a in arrays],
        input_output_aliases={first + i: i for i in range(len(before))},
        compiler_params=params(),
        cost_estimate=pl.CostEstimate(flops=30 * D * F, bytes_accessed=66 * D * F, transcendentals=3 * D * F),
        name=f"adamw{layer}",
    )(factor, *gradients, *arrays, *before)


def solution(mesh):
    def step(x, dy, *arrays):
        wg, wu, wd = arrays[:3]
        gate, up, h1, a0 = forward0(x[0], wg, wu, wd)
        early, late, squares1, dh1 = layer1(h1, dy[0], wg, wu, wd)
        late = lax.all_gather(late, "dp")
        s0, factor = back0(a0, dh1, gate, up, wd, squares1)
        full0 = lax.all_gather(s0, "dp")
        n, blocks = EARLY * FT // FB, FT // FB
        specs = [pl.BlockSpec((1, 3, D, FB), lambda t: (jnp.minimum(t, n - 1) // blocks, 0, 0, jnp.minimum(t, n - 1) % blocks)),
                 pl.BlockSpec((16, 1, 3, 64, FB), lambda t: (0, jnp.maximum(t - n, 0) // blocks, 0, 0, jnp.maximum(t - n, 0) % blocks))]
        new = optimizer(1, kernel_o1, factor, (early, late), specs, arrays, ())
        specs = [pl.BlockSpec((16, 3, 64, FB), lambda t: (0, 0, 0, t))]
        return tuple(optimizer(0, kernel_o0, factor, (full0,), specs, arrays, new))

    return jax.shard_map(
        step,
        mesh=mesh,
        in_specs=(P(("rep", "dp"), None, None),) * 2 + (P(None, None, None),) * 9,
        out_specs=(P("rep", None, None),) * 9,
        check_vma=False,
    )
```
